1024 devices in a mesh: gx: 16 (over y, core), gy: 16 (over z), gz: 4 (over x).
Axes of the slice: x: 4, y: 8, z: 16, core: 2. Of those that a mesh axis runs over, the one named last changes fastest.
Arguments:
- rhs: float32 [4, 128, 128, 512], P(None, 'gx', 'gy', 'gz'), may hold values from -170 to 170
- basis: bfloat16 [4, 8, 128, 128, 512], P(None, None, 'gx', 'gy', 'gz'), may hold values from -6 to 6
- inertia: float32 [128, 128, 512], P('gx', 'gy', 'gz'), may hold values from 0.5 to 2
- helm: float32 [4], replicated, may hold values from 0.2 to 1
- stiffness: float32 [8, 8], replicated, may hold values from -0.05 to 0.6, as said below
Outputs:
- solution: float32 [4, 128, 128, 512], P(None, 'gx', 'gy', 'gz')
- new_basis: bfloat16 [4, 128, 128, 512], P(None, 'gx', 'gy', 'gz')
The draws below stay inside these ranges and needn't reach their ends.
Inputs may be any that keep to these rules, and one draw needn't show every extreme that they name: `stiffness`: symmetric; every diagonal entry exceeds the sum of the magnitudes of the other entries of its row.
All inputs are finite; a program needn't handle non-finite values.
Results may differ from the reference program's by a relative error of at most 0.001.
Values sent between devices are 32-bit elements; how exact they have to be, the bound alone decides.
No kernel may reach another device: no remote copies, remote signals or barrier semaphores. Data moves between devices by JAX's collectives and lax.ppermute only.
A program may use at most 32 MiB of HBM per device.

```python
import math
import jax
import jax.numpy as jnp
from jax import lax

ORDER = 8
SOLVES = 4
KEEP = 8
ITERS = 2
CX = 8
CY = 8
CZ = 128
NX = 128
NY = 128
NZ = 512


def block_levels(key, count, width):
    levels = jax.random.uniform(key, (SOLVES, KEEP, count), jnp.float32, -0.5, 0.5)
    return jnp.repeat(levels, width, axis=2)


def shared_basis(key):
    raw_values = jax.random.normal(jax.random.fold_in(key, 101), (SOLVES, KEEP, NX, NY, NZ), jnp.float32)
    level_x = block_levels(jax.random.fold_in(key, 105), NX // CX, CX)
    level_y = block_levels(jax.random.fold_in(key, 106), NY // CY, CY)
    level_z = block_levels(jax.random.fold_in(key, 107), NZ // CZ, CZ)
    loudness = jnp.exp(level_x[:, :, :, None, None] + level_y[:, :, None, :, None] + level_z[:, :, None, None, :])
    return jnp.clip(raw_values * loudness, -6.0, 6.0)


def draw_basis(key, part):
    return shared_basis(key).astype(jnp.bfloat16)


def draw_rhs(key, part):
    stored = shared_basis(key).astype(jnp.bfloat16).astype(jnp.float32)
    mix_key = jax.random.fold_in(key, 202)
    noise_key = jax.random.fold_in(key, 203)
    ramp_x = jnp.arange(NX, dtype=jnp.float32) / NX
    ramp_y = jnp.arange(NY, dtype=jnp.float32) / NY
    ramp_z = jnp.arange(NZ, dtype=jnp.float32) / NZ
    scaling = 3.0 ** (ramp_x[:, None, None] + ramp_y[None, :, None] + ramp_z[None, None, :] - 1.5)
    mixing = jnp.clip(jax.random.normal(mix_key, (SOLVES, KEEP), jnp.float32), -3.0, 3.0)
    noise = jnp.clip(jax.random.normal(noise_key, (SOLVES, NX, NY, NZ), jnp.float32), -4.0, 4.0)
    return scaling[None] * noise + jnp.einsum('sk,skxyz->sxyz', mixing, stored)


def draw_stiffness(key, part):
    raw_values = jax.random.uniform(jax.random.fold_in(key, 303), (ORDER, ORDER), jnp.float32, -0.05, 0.05)
    off_part = 0.5 * (raw_values + raw_values.T) * (1.0 - jnp.eye(ORDER, dtype=jnp.float32))
    row_weight = jnp.sum(jnp.abs(off_part), axis=1)
    margin = jax.random.uniform(jax.random.fold_in(key, 304), (ORDER,), jnp.float32, 0.08, 0.25)
    return off_part + jnp.diag(row_weight + margin)


def block_scale(rng, extent, cuts, smallest, largest):
    gain = 1.0
    for axis_at, shards_of in cuts:
        draws = jax.random.uniform(jax.random.fold_in(jax.random.fold_in(rng, 6), axis_at), (shards_of,), jnp.float32, smallest / len(cuts), largest / len(cuts))
        gain = gain * jnp.repeat(jnp.exp(draws), extent[axis_at] // shards_of).reshape((-1,) + (1,) * (len(extent) - 1 - axis_at))
    return gain


def setup_inputs(seed: int = 0) -> dict:
    keys = jax.random.split(jax.random.key(seed), 6)
    return {
        "rhs": draw_rhs(jax.random.fold_in(keys[5], 71), 0),
        "basis": draw_basis(jax.random.fold_in(keys[5], 71), 0),
        "inertia": jnp.clip(jnp.exp(math.log(2.0) - 1.3862944 * jax.random.uniform(keys[2], (NX, NY, NZ), jnp.float32) ** block_scale(keys[2], (NX, NY, NZ), ((0, 16), (1, 16), (2, 4)), -0.2, 0.2)), 0.5, 2.0),
        "helm": jnp.clip(jnp.exp(jax.random.uniform(keys[3], (SOLVES,), jnp.float32, math.log(0.2), math.log(1.0))), 0.2, 1.0),
        "stiffness": draw_stiffness(jax.random.fold_in(keys[5], 71), 0),
    }


penalty = 0.15
epsilon = 1e-06
highest = lax.Precision.HIGHEST

def stiffen(vector, stiffness):
    leading, size_a, size_b, size_c = vector.shape
    points = stiffness.shape[0]
    along_a = jnp.einsum('ij,sajbc->saibc', stiffness, vector.reshape(leading, size_a // points, points, size_b, size_c), precision=highest).reshape(vector.shape)
    along_b = jnp.einsum('ij,sabjc->sabic', stiffness, vector.reshape(leading, size_a, size_b // points, points, size_c), precision=highest).reshape(vector.shape)
    along_c = jnp.einsum('ij,sabcj->sabci', stiffness, vector.reshape(leading, size_a, size_b, size_c // points, points), precision=highest).reshape(vector.shape)
    return along_a + along_b + along_c

def face_terms(vector, padded, points):
    accumulated = jnp.zeros_like(vector)
    neighbours = ((1, padded[:, 2:, 1:-1, 1:-1], padded[:, :-2, 1:-1, 1:-1]), (2, padded[:, 1:-1, 2:, 1:-1], padded[:, 1:-1, :-2, 1:-1]), (3, padded[:, 1:-1, 1:-1, 2:], padded[:, 1:-1, 1:-1, :-2]))
    for axis_pos, higher, lower_side in neighbours:
        position = lax.broadcasted_iota(jnp.int32, vector.shape, axis_pos) % points
        accumulated = accumulated + jnp.where(position == points - 1, vector - higher, 0.0)
        accumulated = accumulated + jnp.where(position == 0, vector - lower_side, 0.0)
    return accumulated

def operate(vector, padded, diagonal, stiffness):
    return diagonal * vector + stiffen(vector, stiffness) + penalty * face_terms(vector, padded, stiffness.shape[0])

def reference(rhs, basis, inertia, helm, stiffness):
    point_count = float(rhs.shape[1] * rhs.shape[2] * rhs.shape[3])
    solutions = []
    new_bases = []
    for solve_index in range(SOLVES):
        right_side = rhs[solve_index][None]
        stored = basis[solve_index].astype(jnp.float32)
        diagonal = (helm[solve_index] * inertia)[None]

        def apply_here(vector):
            padded = jnp.pad(vector, ((0, 0), (1, 1), (1, 1), (1, 1)))
            return operate(vector, padded, diagonal, stiffness)
        coefficients = jnp.einsum('kxyz,sxyz->k', stored, right_side, precision=highest) / point_count
        iterate = jnp.einsum('k,kxyz->xyz', coefficients, stored, precision=highest)[None]
        residual = right_side - apply_here(iterate)
        direction = residual
        norm_now = jnp.sum(residual * residual)
        for iteration in range(ITERS):
            image_vec = apply_here(direction)
            step_size = norm_now / jnp.sum(direction * image_vec)
            iterate = iterate + step_size * direction
            residual = residual - step_size * image_vec
            norm_next = jnp.sum(residual * residual)
            direction = residual + norm_next / norm_now * direction
            norm_now = norm_next
        weights = jnp.einsum('kxyz,sxyz->k', stored, iterate, precision=highest) / point_count
        remainder = iterate[0] - jnp.einsum('k,kxyz->xyz', weights, stored, precision=highest)
        spread = jnp.mean(remainder * remainder)
        solutions.append(iterate[0])
        new_bases.append((remainder / jnp.sqrt(spread + epsilon)).astype(jnp.bfloat16))
    return (jnp.stack(solutions), jnp.stack(new_bases))
```

```python
import jax
import jax.numpy as jnp
from jax import lax
from jax.sharding import Mesh
from jax.sharding import PartitionSpec as P

GX = ("gx_0", "gx_1")
PLANE = ("gx_0", "gx_1", "gz")
LINE = ("gy",)

penalty = 0.15
epsilon = 1e-06
max_step = 10.0
highest = lax.Precision.HIGHEST


def total(values):
    shape = values.shape
    flat = values.reshape(-1)
    width = -(-flat.size // 128) * 128
    flat = jnp.pad(flat, (0, width - flat.size)).reshape(1, width)
    for axes in (PLANE, LINE):
        count = lax.axis_size(axes)
        copies = jnp.broadcast_to(flat[None], (count, 1, width))
        flat = lax.optimization_barrier(
            jnp.sum(lax.all_to_all(copies, axes, 0, 0), axis=0)
        )
    size = 1
    for extent in shape:
        size *= extent
    return flat.reshape(-1)[:size].reshape(shape)


def face(x, dim, last):
    length = x.shape[dim]
    return lax.slice_in_dim(x, length - 1 if last else 0, length if last else 1, axis=dim)


def upward(x, axis, dim):
    count = lax.axis_size(axis)
    return lax.ppermute(face(x, dim, True), axis, [(i, i + 1) for i in range(count - 1)])


def downward(x, axis, dim):
    count = lax.axis_size(axis)
    return lax.ppermute(face(x, dim, False), axis, [(i + 1, i) for i in range(count - 1)])


SIDES = (("gz", 3), ("gy", 2), (GX, 1))


def halo(x):
    return [(dim, upward(x, axis, dim), downward(x, axis, dim)) for axis, dim in SIDES]


def outer(x, faces):
    added = jnp.zeros_like(x)
    for dim, low, high in faces:
        position = lax.broadcasted_iota(jnp.int32, x.shape, dim)
        added = added + jnp.where(position == 0, low, 0.0)
        added = added + jnp.where(position == x.shape[dim] - 1, high, 0.0)
    return -penalty * added


def matrices(stiffness, size_z):
    points = stiffness.shape[0]
    row = lax.broadcasted_iota(jnp.int32, (points, points), 0)
    col = lax.broadcasted_iota(jnp.int32, (points, points), 1)
    ends = (row == col) & ((row == 0) | (row == points - 1))
    closed = stiffness + jnp.where(ends, penalty, 0.0)
    eye = jnp.where(row == col, 1.0, 0.0)
    plane = (closed[:, None, :, None] * eye[None, :, None, :]
             + eye[:, None, :, None] * closed[None, :, None, :]).reshape(points * points, points * points)
    row = lax.broadcasted_iota(jnp.int32, (size_z, size_z), 0)
    col = lax.broadcasted_iota(jnp.int32, (size_z, size_z), 1)
    spread_out = jnp.tile(closed, (size_z // points, size_z // points))
    line = jnp.where(row // points == col // points, spread_out, 0.0)
    edge = (jnp.abs(row - col) == 1) & (row // points != col // points)
    return plane, jnp.where(edge, -penalty, line)


def dots(a, b):
    return jnp.sum(a * b, axis=(1, 2, 3))


def per_solve(values):
    return values[:, None, None, None]


def on_device(rhs, basis, inertia, helm, stiffness):
    solves, size_x, size_y, size_z = rhs.shape
    point_count = float(rhs[0].size * lax.axis_size(PLANE + LINE))
    diagonal = helm[:, None, None, None] * inertia[None]
    plane, line = matrices(stiffness, size_z)

    def inner(v):
        flat = v.reshape(solves, size_x * size_y, size_z)
        along = jnp.einsum("ij,sjc->sic", plane, flat, precision=highest)
        along = along + jnp.einsum("sjc,cd->sjd", flat, line, precision=highest)
        return diagonal * v + along.reshape(v.shape)

    def combine(weights):
        return jnp.einsum("sk,skxyz->sxyz", weights, basis, precision=highest)

    coef = total(jnp.einsum("skxyz,sxyz->sk", basis, rhs, precision=highest)) / point_count
    start = combine(coef)
    resid = rhs - inner(start) - outer(start, halo(start))
    image = inner(resid) + outer(resid, halo(resid))

    lows = [upward(image, axis, dim) for axis, dim in SIDES]
    cubic = dots(image, inner(image))
    for (_, dim), low in zip(SIDES, lows):
        cubic = cubic - 2.0 * penalty * dots(face(image, dim, False), low)
    pair = jnp.stack([resid, image], axis=1)
    moment = jnp.einsum("skxyz,smxyz->smk", basis, pair, precision=highest)
    gram = jnp.einsum("skxyz,slxyz->skl", basis, basis, preferred_element_type=jnp.float32)
    powers = jnp.stack([dots(resid, resid), dots(resid, image), dots(image, image), cubic], axis=1)
    sums = total(jnp.concatenate(
        [powers, moment.reshape(solves, -1), gram.reshape(solves, -1)], axis=1)) / point_count
    keep = coef.shape[1]
    mu0, mu1, mu2, mu3 = (sums[:, i] for i in range(4))
    moment = sums[:, 4:4 + 2 * keep].reshape(solves, 2, keep)
    gram = sums[:, 4 + 2 * keep:].reshape(solves, keep, keep)

    step_0 = mu0 / mu1
    next_0 = jnp.maximum(step_0 * step_0 * mu2 - mu0, 0.0)
    ratio = next_0 / mu0
    grown = 1.0 + ratio
    curvature = grown * grown * mu1 - 2.0 * grown * step_0 * mu2 + step_0 * step_0 * mu3
    step_1 = jnp.where(curvature * max_step > next_0, next_0 / curvature, max_step)
    of_resid = step_0 + step_1 * grown
    of_image = -step_1 * step_0
    change = of_resid[:, None] * moment[:, 0] + of_image[:, None] * moment[:, 1]
    weights = jnp.einsum("skl,sl->sk", gram, coef, precision=highest) + change
    left = coef - weights
    spread = (
        jnp.einsum("sk,skl,sl->s", left, gram, left, precision=highest)
        + 2.0 * jnp.sum(left * change, axis=1)
        + of_resid * of_resid * mu0 + 2.0 * of_resid * of_image * mu1 + of_image * of_image * mu2
    )
    iterate = start + per_solve(of_resid) * resid + per_solve(of_image) * image
    remainder = iterate - combine(weights)
    new_basis = (remainder * per_solve(lax.rsqrt(spread + epsilon))).astype(jnp.bfloat16)
    return (iterate, new_basis)


def solution(mesh):
    torus = Mesh(
        mesh.devices.reshape(mesh.shape["gx"] // 2, 2, mesh.shape["gy"], mesh.shape["gz"]),
        ("gx_0", "gx_1", "gy", "gz"),
    )
    placed = (P(None, GX, "gy", "gz"), P(None, None, GX, "gy", "gz"), P(GX, "gy", "gz"), P(), P())
    return jax.shard_map(
        on_device,
        mesh=torus,
        in_specs=placed,
        out_specs=(P(None, GX, "gy", "gz"), P(None, GX, "gy", "gz")),
        check_vma=False,
    )
```

```python
import jax
import jax.numpy as jnp
from jax import lax
from jax.experimental import pallas as pl
from jax.experimental.pallas import tpu as pltpu
from jax.sharding import Mesh
from jax.sharding import PartitionSpec as P

GX = ("gx_0", "gx_1")
PLANE = ("gx_0", "gx_1", "gz")
LINE = ("gy",)

penalty = 0.15
epsilon = 1e-06
max_step = 10.0
f32 = jnp.float32
S, K, X, Y, Z = 4, 8, 8, 8, 128
SX, SK, SXY = S * X, S * K, S * X * Y
DIAGONALS = 5
ROWS = 2 * SK + 16 + DIAGONALS * SK


def mm(a, b, left=1, right=0):
    return lax.dot_general(
        a, b, (((left,), (right,)), ((), ())), precision=lax.Precision.HIGHEST, preferred_element_type=f32
    )


def iota(shape, dim):
    return lax.broadcasted_iota(jnp.int32, shape, dim)


def where(mask):
    return jnp.where(mask, 1.0, 0.0).astype(f32)


def ends():
    row, col = iota((8, Z), 0), iota((8, Z), 1)
    return where(((row == 0) & (col == 0)) | ((row == 1) & (col == Z - 1)))


def stack_rows(first, second):
    row = iota((8, first.shape[1]), 0)
    return jnp.where(row == 0, first, jnp.where(row == 1, second, 0.0))


def spread(first, second):
    return mm(stack_rows(first, second), ends(), 0, 0)


def laplace(v, inertia, helm_ref, plane, line):
    along = mm(v, line)
    parts = []
    for s in range(S):
        part = v[s * X * Y:(s + 1) * X * Y]
        parts.append(helm_ref[s] * inertia * part + mm(plane, part))
    return along + jnp.concatenate(parts, axis=0)


def at_x(low, high):
    x = iota((S, X, Y, Z), 1)
    return jnp.where(x == 0, low[:, None], jnp.where(x == X - 1, high[:, None], 0.0))


def at_y(low, high):
    y = iota((S, X, Y, Z), 2)
    low, high = low.reshape(S, X, 1, Z), high.reshape(S, X, 1, Z)
    return jnp.where(y == 0, low, jnp.where(y == Y - 1, high, 0.0))


def column(values, at):
    return values[:, at:at + 1]


def weighted(weights, basis_ref, s):
    out = None
    for k in range(K):
        term = column(weights, s * K + k) * basis_ref[s, k].astype(f32).reshape(X * Y, Z)
        out = term if out is None else out + term
    return out


def row_sum(product):
    return jnp.sum(product.reshape(X * Y, Z), axis=0, keepdims=True)


def lane_sums(rows):
    return mm(jnp.ones((8, Z), f32), rows, 1, 1)[0:1]


def coef_kernel(rhs_ref, basis_ref, out_ref):
    rows = []
    for s in range(S):
        right = rhs_ref[s]
        for k in range(K):
            rows.append(row_sum(basis_ref[s, k].astype(f32) * right))
    rows = jnp.concatenate(rows + [jnp.zeros((Z - SK, Z), f32)], axis=0)
    out_ref[...] = jnp.broadcast_to(lane_sums(rows)[None], out_ref.shape)


def fold_kernel(in_ref, out_ref):
    out_ref[...] = jnp.broadcast_to(jnp.sum(in_ref[...], axis=0, keepdims=True), out_ref.shape)


def build(stiffness):
    row, col = iota((8, 8), 0), iota((8, 8), 1)
    closed = stiffness + jnp.where((row == col) & ((row == 0) | (row == 7)), penalty, 0.0)
    low = where(iota((X * Y, 8), 0) % 8 == iota((X * Y, 8), 1))
    high = where(iota((X * Y, 8), 0) // 8 == iota((X * Y, 8), 1))
    row, col = iota((X * Y, X * Y), 0), iota((X * Y, X * Y), 1)
    along_x = mm(mm(high, closed), high, 1, 1) * where(row % 8 == col % 8)
    along_y = mm(mm(low, closed), low, 1, 1) * where(row // 8 == col // 8)
    low = where(iota((Z, 8), 0) % 8 == iota((Z, 8), 1))
    row, col = iota((Z, Z), 0), iota((Z, Z), 1)
    same = row // 8 == col // 8
    line = mm(mm(low, closed), low, 1, 1) * where(same)
    line = line - penalty * where((jnp.abs(row - col) == 1) & ~same)
    return along_x + along_y, line


def start_kernel(scale, sums_ref, basis_ref, rhs_ref, inertia_ref, helm_ref, stiffness_ref,
                 coef_ref, x0_ref, q_ref, plane_ref, line_ref, up_ref, down_ref):
    plane, line = build(stiffness_ref[...])
    plane_ref[...] = plane
    line_ref[...] = line
    coef = jnp.sum(sums_ref[...], axis=0) * scale
    coef_ref[...] = coef
    x0 = jnp.concatenate([weighted(coef, basis_ref, s) for s in range(S)], axis=0)
    inertia = inertia_ref[...].reshape(X * Y, Z)
    q = rhs_ref[...].reshape(SXY, Z) - laplace(x0, inertia, helm_ref, plane, line)
    x0, q = x0.reshape(S, X, Y, Z), q.reshape(S, X, Y, Z)
    x0_ref[...] = x0
    q_ref[...] = q
    up_ref[0] = x0[:, X - 1]
    up_ref[1] = q[:, X - 1]
    down_ref[0] = x0[:, 0]
    down_ref[1] = q[:, 0]


def y_kernel(x0_ref, q_ref, xlo_ref, xhi_ref, up_ref, down_ref):
    for out_ref, y in ((up_ref, Y - 1), (down_ref, 0)):
        for s in range(S):
            low, high = xlo_ref[0, s, y:y + 1, :], xhi_ref[0, s, y:y + 1, :]
            for x in range(X):
                i = s * X + x
                out_ref[i:i + 1, :] = x0_ref[s, x, y:y + 1, :]
                q = q_ref[s, x, y:y + 1, :]
                if x == 0:
                    q = q + penalty * low
                if x == X - 1:
                    q = q + penalty * high
                out_ref[SX + i:SX + i + 1, :] = q
            out_ref[2 * SX + s:2 * SX + s + 1, :] = low
            out_ref[2 * SX + S + s:2 * SX + S + s + 1, :] = high


def z_kernel(x0_ref, q_ref, xlo_ref, xhi_ref, ylo_ref, yhi_ref, q2_ref, up_ref, down_ref):
    q = q_ref[...] + penalty * (at_x(xlo_ref[0], xhi_ref[0]) + at_y(ylo_ref[0:SX], yhi_ref[0:SX]))
    q2_ref[...] = q
    rows = jnp.concatenate(
        [x0_ref[...].reshape(SXY, Z), q.reshape(SXY, Z), xlo_ref[0].reshape(SX, Z), xhi_ref[0].reshape(SX, Z),
         ylo_ref[0:SX], yhi_ref[0:SX]], axis=0)
    picked = mm(ends(), rows, 1, 1)
    down_ref[...] = picked[0:1]
    up_ref[...] = picked[1:2]


def image_kernel(x0_ref, q2_ref, xlo_ref, xhi_ref, ylo_ref, yhi_ref, zlo_ref, zhi_ref, zup_ref, zdown_ref,
                 inside_ref, inertia_ref, helm_ref, plane_ref, line_ref,
                 r0_ref, v_ref, vx_ref, vy_ref, vz_ref, vz0_ref):
    zlo, zhi = zlo_ref[...], zhi_ref[...]
    put = spread(zlo, zhi)
    x0 = x0_ref[...]
    r0 = q2_ref[...].reshape(SXY, Z) + penalty * put[0:SXY]
    at = 2 * SXY
    rzl = inside_ref[4] * (zlo[:, SXY:at] + penalty * zdown_ref[:, 0:SXY])
    rzh = inside_ref[5] * (zhi[:, SXY:at] + penalty * zup_ref[:, 0:SXY])
    ends_y = []
    for y in (0, Y - 1):
        ends_y.append(jnp.concatenate(
            [x0_ref[s, x, y:y + 1, :] for s in range(S) for x in range(X)], axis=0))
    ryl = inside_ref[2] * (ylo_ref[SX:2 * SX] + penalty * (ends_y[0] + put[at + 2 * SX:at + 3 * SX]))
    ryh = inside_ref[3] * (yhi_ref[SX:2 * SX] + penalty * (ends_y[1] + put[at + 3 * SX:at + 4 * SX]))
    y = iota((S, Y, Z), 1)

    def layer(flag, q, own, first, columns):
        low, high = ylo_ref[first:first + S].reshape(S, 1, Z), yhi_ref[first:first + S].reshape(S, 1, Z)
        lines = jnp.where(y == 0, low, jnp.where(y == Y - 1, high, 0.0))
        return flag * (q + penalty * (own + lines + columns.reshape(S, Y, Z)))

    rxl = layer(inside_ref[0], xlo_ref[1], x0[:, 0], 2 * SX, put[at:at + SX])
    rxh = layer(inside_ref[1], xhi_ref[1], x0[:, X - 1], 2 * SX + S, put[at + SX:at + 2 * SX])
    around = at_x(rxl, rxh) + at_y(ryl, ryh)
    v = laplace(r0, inertia_ref[...].reshape(X * Y, Z), helm_ref, plane_ref[...], line_ref[...])
    v = v - penalty * (around.reshape(SXY, Z) + spread(rzl, rzh))
    picked = mm(ends(), v, 1, 1)
    vz0_ref[...] = picked[0:1]
    vz_ref[...] = picked[1:2]
    v = v.reshape(S, X, Y, Z)
    r0_ref[...] = r0.reshape(S, X, Y, Z)
    v_ref[...] = v
    vx_ref[...] = v[:, X - 1]
    for s in range(S):
        for x in range(X):
            vy_ref[s * X + x:s * X + x + 1, :] = v_ref[s, x, Y - 1:Y, :]


def moment_kernel(r0_ref, v_ref, basis_ref, inertia_ref, helm_ref, plane_ref, line_ref, out_ref):
    v_all = v_ref[...].reshape(SXY, Z)
    w_all = laplace(v_all, inertia_ref[...].reshape(X * Y, Z), helm_ref, plane_ref[...], line_ref[...])
    for s in range(S):
        r, v = r0_ref[s], v_ref[s]
        w = w_all[s * X * Y:(s + 1) * X * Y].reshape(X, Y, Z)
        at = 2 * SK + 4 * s
        for j, product in enumerate((r * r, r * v, v * v, v * w)):
            out_ref[at + j:at + j + 1, :] = row_sum(product)
        for k in range(K):
            b = basis_ref[s, k].astype(f32)
            i = s * K + k
            out_ref[i:i + 1, :] = row_sum(b * r)
            out_ref[SK + i:SK + i + 1, :] = row_sum(b * v)
            for d in range(DIAGONALS):
                at = 2 * SK + 16 + d * SK + i
                out_ref[at:at + 1, :] = row_sum(b * basis_ref[s, (k + d) % K].astype(f32))
    out_ref[ROWS:, :] = jnp.zeros((256 - ROWS, Z), f32)


def cross_kernel(rows_ref, v_ref, vz0_ref, xlo_ref, ylo_ref, zlo_ref, out_ref):
    rows = rows_ref[...]
    row = iota((256, Z), 0)
    z = vz0_ref[...] * zlo_ref[...]
    for s in range(S):
        crossing = jnp.sum(v_ref[s, 0] * xlo_ref[s], axis=0, keepdims=True)
        for x in range(X):
            crossing = crossing + v_ref[s, x, 0:1, :] * ylo_ref[s * X + x:s * X + x + 1, :]
        part = z[:, s * X * Y:(s + 1) * X * Y]
        crossing = crossing + jnp.concatenate([part, jnp.zeros((1, Z - X * Y), f32)], axis=1)
        rows = rows - jnp.where(row == 2 * SK + 4 * s + 3, 2.0 * penalty * crossing, 0.0)
    out_ref[...] = jnp.broadcast_to(lane_sums(rows)[None], out_ref.shape)


def final_kernel(scale, sums_ref, coef_ref, x0_ref, r0_ref, v_ref, basis_ref, out_ref, new_ref):
    sums = jnp.broadcast_to(jnp.sum(sums_ref[...], axis=0) * scale, (8, 256))
    g0, g1 = sums[:, 0:SK], sums[:, SK:2 * SK]
    powers = sums[:, 2 * SK:2 * SK + 16]
    row, col = iota((16, 4 * SK), 0), iota((16, 4 * SK), 1)
    powers = mm(powers, where(row == 4 * ((col % SK) // K) + col // SK))
    mu0, mu1, mu2, mu3 = (powers[:, j * SK:(j + 1) * SK] for j in range(4))
    gram = [sums[:, 2 * SK + 16 + d * SK:2 * SK + 16 + (d + 1) * SK] for d in range(DIAGONALS)]
    coef = jnp.broadcast_to(coef_ref[:, 0:SK], (8, SK))

    row, col = iota((SK, SK), 0), iota((SK, SK), 1)
    same = row // K == col // K
    turn = [where(same & ((col % K + d) % K == row % K)) for d in range(DIAGONALS)]
    back = [where(same & ((row % K + d) % K == col % K)) for d in range(DIAGONALS)]
    block = where(same)

    def gram_times(u):
        out = gram[0] * u
        for d in range(1, DIAGONALS):
            out = out + gram[d] * mm(u, turn[d])
        for d in range(1, DIAGONALS - 1):
            out = out + mm(gram[d] * u, back[d])
        return out

    step_0 = mu0 / mu1
    next_0 = jnp.maximum(step_0 * step_0 * mu2 - mu0, 0.0)
    grown = 1.0 + next_0 / mu0
    curvature = grown * grown * mu1 - 2.0 * grown * step_0 * mu2 + step_0 * step_0 * mu3
    step_1 = jnp.where(curvature * max_step > next_0, next_0 / curvature, max_step)
    of_r = step_0 + step_1 * grown
    of_v = -step_1 * step_0
    change = of_r * g0 + of_v * g1
    weights = gram_times(coef) + change
    left = coef - weights
    square = mm(left * gram_times(left) + 2.0 * left * change, block)
    square = square + of_r * of_r * mu0 + 2.0 * of_r * of_v * mu1 + of_v * of_v * mu2
    inverse = lax.rsqrt(square + epsilon)
    for s in range(S):
        at = s * K
        x = x0_ref[s].reshape(X * Y, Z) + column(of_r[0:1], at) * r0_ref[s].reshape(X * Y, Z)
        x = x + column(of_v[0:1], at) * v_ref[s].reshape(X * Y, Z)
        out_ref[s] = x.reshape(X, Y, Z)
        rest = (x - weighted(weights[0:1], basis_ref, s)) * column(inverse[0:1], at)
        new_ref[s] = rest.reshape(X, Y, Z).astype(jnp.bfloat16)


def shaped(*shape, dtype=f32):
    return jax.ShapeDtypeStruct(shape, dtype)


def call(kernel, outs, args, small=()):
    vmem, smem = pl.BlockSpec(memory_space=pltpu.VMEM), pl.BlockSpec(memory_space=pltpu.SMEM)
    return pl.pallas_call(
        kernel,
        out_shape=outs,
        in_specs=[smem if i in small else vmem for i in range(len(args))],
        out_specs=jax.tree.map(lambda _: vmem, outs),
    )(*args)


def total(copies):
    width = copies.shape[2]
    copies = lax.all_to_all(copies, PLANE, 0, 0)
    copies = call(fold_kernel, shaped(lax.axis_size(LINE), 1, width), (copies,))
    return lax.all_to_all(copies, LINE, 0, 0)


def upward(x, axis):
    return lax.ppermute(x, axis, [(i, i + 1) for i in range(lax.axis_size(axis) - 1)])


def downward(x, axis):
    return lax.ppermute(x, axis, [(i + 1, i) for i in range(lax.axis_size(axis) - 1)])


def on_device(rhs, basis, inertia, helm, stiffness):
    scale = 1.0 / float(rhs[0].size * lax.axis_size(PLANE + LINE))
    peers = lax.axis_size(PLANE)
    field = shaped(S, X, Y, Z)

    copies = call(coef_kernel, shaped(peers, 1, Z), (rhs, basis))
    sums = total(copies)

    def start(*refs):
        start_kernel(scale, *refs)

    coef, x0, q, plane, line, up, down = call(
        start,
        (shaped(1, Z), field, field, shaped(X * Y, X * Y), shaped(Z, Z), shaped(2, S, Y, Z), shaped(2, S, Y, Z)),
        (sums, basis, rhs, inertia, helm, stiffness), small=(4,))
    xlo, xhi = upward(up, GX), downward(down, GX)
    up, down = call(y_kernel, (shaped(2 * SX + 8, Z),) * 2, (x0, q, xlo, xhi))
    ylo, yhi = upward(up, "gy"), downward(down, "gy")
    q2, zup, zdown = call(
        z_kernel, (field, shaped(1, 640), shaped(1, 640)), (x0, q, xlo, xhi, ylo, yhi))
    zlo, zhi = upward(zup, "gz"), downward(zdown, "gz")

    places = [(lax.axis_index(axis), lax.axis_size(axis)) for axis in (GX, "gy", "gz")]
    inside = jnp.stack([jnp.where(test, 1.0, 0.0) for i, n in places for test in (i > 0, i < n - 1)])
    r0, v, vx, vy, vz, vz0 = call(
        image_kernel,
        (field, field, shaped(S, Y, Z), shaped(SX, Z), shaped(1, SXY), shaped(1, SXY)),
        (x0, q2, xlo, xhi, ylo, yhi, zlo, zhi, zup, zdown, inside, inertia, helm, plane, line), small=(10, 12))
    lows = [upward(a, axis) for a, axis in ((vx, GX), (vy, "gy"), (vz, "gz"))]
    rows = call(moment_kernel, shaped(256, Z), (r0, v, basis, inertia, helm, plane, line), small=(4,))
    copies = call(cross_kernel, shaped(peers, 1, 256), (rows, v, vz0, *lows))
    sums = total(copies)

    def final(*refs):
        final_kernel(scale, *refs)

    return call(final, (field, shaped(S, X, Y, Z, dtype=jnp.bfloat16)), (sums, coef, x0, r0, v, basis))


def solution(mesh):
    torus = Mesh(
        mesh.devices.reshape(mesh.shape["gx"] // 2, 2, mesh.shape["gy"], mesh.shape["gz"]),
        ("gx_0", "gx_1", "gy", "gz"),
    )
    placed = (P(None, GX, "gy", "gz"), P(None, None, GX, "gy", "gz"), P(GX, "gy", "gz"), P(), P())
    return jax.shard_map(
        on_device,
        mesh=torus,
        in_specs=placed,
        out_specs=(P(None, GX, "gy", "gz"), P(None, GX, "gy", "gz")),
        check_vma=False,
    )
```

```python
import jax
import jax.numpy as jnp
from jax import lax
from jax.experimental import pallas as pl
from jax.experimental.pallas import tpu as pltpu
from jax.sharding import Mesh
from jax.sharding import PartitionSpec as P

GX = ("gx_0", "gx_1")
PLANE = ("gx_0", "gx_1", "gz")
LINE = ("gy",)

penalty = 0.15
epsilon = 1e-06
max_step = 10.0
f32 = jnp.float32
S, K, X, Y, Z = 4, 8, 8, 8, 128
SX, SK, SXY = S * X, S * K, S * X * Y
DIAGONALS = 5
ROWS = 2 * SK + 16 + DIAGONALS * SK


def mm(a, b, left=1, right=0):
    return lax.dot_general(
        a, b, (((left,), (right,)), ((), ())), precision=lax.Precision.HIGHEST, preferred_element_type=f32
    )


def iota(shape, dim):
    return lax.broadcasted_iota(jnp.int32, shape, dim)


def where(mask):
    return jnp.where(mask, 1.0, 0.0).astype(f32)


def ends():
    row, col = iota((8, Z), 0), iota((8, Z), 1)
    return where(((row == 0) & (col == 0)) | ((row == 1) & (col == Z - 1)))


def stack_rows(first, second):
    row = iota((8, first.shape[1]), 0)
    return jnp.where(row == 0, first, jnp.where(row == 1, second, 0.0))


def spread(first, second):
    return mm(stack_rows(first, second), ends(), 0, 0)


def laplace(v, inertia, helm_ref, plane, line):
    along = mm(v, line)
    parts = []
    for s in range(S):
        part = v[s * X * Y:(s + 1) * X * Y]
        parts.append(helm_ref[s] * inertia * part + mm(plane, part))
    return along + jnp.concatenate(parts, axis=0)


def at_x(low, high):
    x = iota((S, X, Y, Z), 1)
    return jnp.where(x == 0, low[:, None], jnp.where(x == X - 1, high[:, None], 0.0))


def at_y(low, high):
    y = iota((S, X, Y, Z), 2)
    low, high = low.reshape(S, X, 1, Z), high.reshape(S, X, 1, Z)
    return jnp.where(y == 0, low, jnp.where(y == Y - 1, high, 0.0))


def column(values, at):
    return values[:, at:at + 1]


def weighted(weights, basis_ref, s):
    out = None
    for k in range(K):
        term = column(weights, s * K + k) * basis_ref[s, k].astype(f32).reshape(X * Y, Z)
        out = term if out is None else out + term
    return out


def row_sum(product):
    return jnp.sum(product.reshape(X * Y, Z), axis=0, keepdims=True)


def lane_sums(rows):
    return mm(jnp.ones((8, Z), f32), rows, 1, 1)[0:1]


def coef_kernel(rhs_ref, basis_ref, out_ref):
    rows = []
    for s in range(S):
        right = rhs_ref[s]
        for k in range(K):
            rows.append(row_sum(basis_ref[s, k].astype(f32) * right))
    rows = jnp.concatenate(rows + [jnp.zeros((Z - SK, Z), f32)], axis=0)
    out_ref[...] = jnp.broadcast_to(lane_sums(rows)[None], out_ref.shape)


def fold_kernel(in_ref, out_ref):
    out_ref[...] = jnp.broadcast_to(jnp.sum(in_ref[...], axis=0, keepdims=True), out_ref.shape)


def build(stiffness):
    row, col = iota((8, 8), 0), iota((8, 8), 1)
    closed = stiffness + jnp.where((row == col) & ((row == 0) | (row == 7)), penalty, 0.0)
    low = where(iota((X * Y, 8), 0) % 8 == iota((X * Y, 8), 1))
    high = where(iota((X * Y, 8), 0) // 8 == iota((X * Y, 8), 1))
    row, col = iota((X * Y, X * Y), 0), iota((X * Y, X * Y), 1)
    along_x = mm(mm(high, closed), high, 1, 1) * where(row % 8 == col % 8)
    along_y = mm(mm(low, closed), low, 1, 1) * where(row // 8 == col // 8)
    low = where(iota((Z, 8), 0) % 8 == iota((Z, 8), 1))
    row, col = iota((Z, Z), 0), iota((Z, Z), 1)
    same = row // 8 == col // 8
    line = mm(mm(low, closed), low, 1, 1) * where(same)
    line = line - penalty * where((jnp.abs(row - col) == 1) & ~same)
    return along_x + along_y, line


def start_kernel(scale, sums_ref, basis_ref, rhs_ref, inertia_ref, helm_ref, stiffness_ref,
                 coef_ref, x0_ref, q_ref, plane_ref, line_ref, up_ref, down_ref):
    plane, line = build(stiffness_ref[...])
    plane_ref[...] = plane
    line_ref[...] = line
    coef = jnp.sum(sums_ref[...], axis=0) * scale
    coef_ref[...] = coef
    x0 = jnp.concatenate([weighted(coef, basis_ref, s) for s in range(S)], axis=0)
    inertia = inertia_ref[...].reshape(X * Y, Z)
    q = rhs_ref[...].reshape(SXY, Z) - laplace(x0, inertia, helm_ref, plane, line)
    x0, q = x0.reshape(S, X, Y, Z), q.reshape(S, X, Y, Z)
    x0_ref[...] = x0
    q_ref[...] = q
    up_ref[0] = x0[:, X - 1]
    up_ref[1] = q[:, X - 1]
    down_ref[0] = x0[:, 0]
    down_ref[1] = q[:, 0]


def y_kernel(x0_ref, q_ref, xlo_ref, xhi_ref, up_ref, down_ref):
    for out_ref, y in ((up_ref, Y - 1), (down_ref, 0)):
        for s in range(S):
            low, high = xlo_ref[0, s, y:y + 1, :], xhi_ref[0, s, y:y + 1, :]
            for x in range(X):
                i = s * X + x
                out_ref[i:i + 1, :] = x0_ref[s, x, y:y + 1, :]
                q = q_ref[s, x, y:y + 1, :]
                if x == 0:
                    q = q + penalty * low
                if x == X - 1:
                    q = q + penalty * high
                out_ref[SX + i:SX + i + 1, :] = q
            out_ref[2 * SX + s:2 * SX + s + 1, :] = low
            out_ref[2 * SX + S + s:2 * SX + S + s + 1, :] = high


def z_kernel(x0_ref, q_ref, xlo_ref, xhi_ref, ylo_ref, yhi_ref, q2_ref, up_ref, down_ref):
    q = q_ref[...] + penalty * (at_x(xlo_ref[0], xhi_ref[0]) + at_y(ylo_ref[0:SX], yhi_ref[0:SX]))
    q2_ref[...] = q
    rows = jnp.concatenate(
        [x0_ref[...].reshape(SXY, Z), q.reshape(SXY, Z), xlo_ref[0].reshape(SX, Z), xhi_ref[0].reshape(SX, Z),
         ylo_ref[0:SX], yhi_ref[0:SX]], axis=0)
    picked = mm(ends(), rows, 1, 1)
    down_ref[...] = picked[0:1]
    up_ref[...] = picked[1:2]


def image_kernel(x0_ref, q2_ref, xlo_ref, xhi_ref, ylo_ref, yhi_ref, zlo_ref, zhi_ref, zup_ref, zdown_ref,
                 inside_ref, inertia_ref, helm_ref, plane_ref, line_ref,
                 r0_ref, v_ref, vx_ref, vy_ref, vz_ref, vz0_ref):
    zlo, zhi = zlo_ref[...], zhi_ref[...]
    put = spread(zlo, zhi)
    x0 = x0_ref[...]
    r0 = q2_ref[...].reshape(SXY, Z) + penalty * put[0:SXY]
    at = 2 * SXY
    rzl = inside_ref[4] * (zlo[:, SXY:at] + penalty * zdown_ref[:, 0:SXY])
    rzh = inside_ref[5] * (zhi[:, SXY:at] + penalty * zup_ref[:, 0:SXY])
    ends_y = []
    for y in (0, Y - 1):
        ends_y.append(jnp.concatenate(
            [x0_ref[s, x, y:y + 1, :] for s in range(S) for x in range(X)], axis=0))
    ryl = inside_ref[2] * (ylo_ref[SX:2 * SX] + penalty * (ends_y[0] + put[at + 2 * SX:at + 3 * SX]))
    ryh = inside_ref[3] * (yhi_ref[SX:2 * SX] + penalty * (ends_y[1] + put[at + 3 * SX:at + 4 * SX]))
    y = iota((S, Y, Z), 1)

    def layer(flag, q, own, first, columns):
        low, high = ylo_ref[first:first + S].reshape(S, 1, Z), yhi_ref[first:first + S].reshape(S, 1, Z)
        lines = jnp.where(y == 0, low, jnp.where(y == Y - 1, high, 0.0))
        return flag * (q + penalty * (own + lines + columns.reshape(S, Y, Z)))

    rxl = layer(inside_ref[0], xlo_ref[1], x0[:, 0], 2 * SX, put[at:at + SX])
    rxh = layer(inside_ref[1], xhi_ref[1], x0[:, X - 1], 2 * SX + S, put[at + SX:at + 2 * SX])
    around = at_x(rxl, rxh) + at_y(ryl, ryh)
    v = laplace(r0, inertia_ref[...].reshape(X * Y, Z), helm_ref, plane_ref[...], line_ref[...])
    v = v - penalty * (around.reshape(SXY, Z) + spread(rzl, rzh))
    picked = mm(ends(), v, 1, 1)
    vz0_ref[...] = picked[0:1]
    vz_ref[...] = picked[1:2]
    v = v.reshape(S, X, Y, Z)
    r0_ref[...] = r0.reshape(S, X, Y, Z)
    v_ref[...] = v
    vx_ref[...] = v[:, X - 1]
    for s in range(S):
        for x in range(X):
            vy_ref[s * X + x:s * X + x + 1, :] = v_ref[s, x, Y - 1:Y, :]


def moment_kernel(r0_ref, v_ref, basis_ref, inertia_ref, helm_ref, plane_ref, line_ref, out_ref):
    v_all = v_ref[...].reshape(SXY, Z)
    w_all = laplace(v_all, inertia_ref[...].reshape(X * Y, Z), helm_ref, plane_ref[...], line_ref[...])
    for s in range(S):
        r, v = r0_ref[s], v_ref[s]
        w = w_all[s * X * Y:(s + 1) * X * Y].reshape(X, Y, Z)
        at = 2 * SK + 4 * s
        for j, product in enumerate((r * r, r * v, v * v, v * w)):
            out_ref[at + j:at + j + 1, :] = row_sum(product)
        for k in range(K):
            b = basis_ref[s, k].astype(f32)
            i = s * K + k
            out_ref[i:i + 1, :] = row_sum(b * r)
            out_ref[SK + i:SK + i + 1, :] = row_sum(b * v)
            for d in range(DIAGONALS):
                at = 2 * SK + 16 + d * SK + i
                out_ref[at:at + 1, :] = row_sum(b * basis_ref[s, (k + d) % K].astype(f32))
    out_ref[ROWS:, :] = jnp.zeros((256 - ROWS, Z), f32)


def cross_kernel(rows_ref, v_ref, vz0_ref, xlo_ref, ylo_ref, zlo_ref, out_ref):
    rows = rows_ref[...]
    row = iota((256, Z), 0)
    z = vz0_ref[...] * zlo_ref[...]
    for s in range(S):
        crossing = jnp.sum(v_ref[s, 0] * xlo_ref[s], axis=0, keepdims=True)
        for x in range(X):
            crossing = crossing + v_ref[s, x, 0:1, :] * ylo_ref[s * X + x:s * X + x + 1, :]
        part = z[:, s * X * Y:(s + 1) * X * Y]
        crossing = crossing + jnp.concatenate([part, jnp.zeros((1, Z - X * Y), f32)], axis=1)
        rows = rows - jnp.where(row == 2 * SK + 4 * s + 3, 2.0 * penalty * crossing, 0.0)
    out_ref[...] = jnp.broadcast_to(lane_sums(rows)[None], out_ref.shape)


def final_kernel(scale, sums_ref, coef_ref, x0_ref, r0_ref, v_ref, basis_ref, out_ref, new_ref):
    sums = jnp.broadcast_to(jnp.sum(sums_ref[...], axis=0) * scale, (8, 256))
    g0, g1 = sums[:, 0:SK], sums[:, SK:2 * SK]
    powers = sums[:, 2 * SK:2 * SK + 16]
    row, col = iota((16, 4 * SK), 0), iota((16, 4 * SK), 1)
    powers = mm(powers, where(row == 4 * ((col % SK) // K) + col // SK))
    mu0, mu1, mu2, mu3 = (powers[:, j * SK:(j + 1) * SK] for j in range(4))
    gram = [sums[:, 2 * SK + 16 + d * SK:2 * SK + 16 + (d + 1) * SK] for d in range(DIAGONALS)]
    coef = jnp.broadcast_to(coef_ref[:, 0:SK], (8, SK))

    row, col = iota((SK, SK), 0), iota((SK, SK), 1)
    same = row // K == col // K
    turn = [where(same & ((col % K + d) % K == row % K)) for d in range(DIAGONALS)]
    back = [where(same & ((row % K + d) % K == col % K)) for d in range(DIAGONALS)]
    block = where(same)

    def gram_times(u):
        out = gram[0] * u
        for d in range(1, DIAGONALS):
            out = out + gram[d] * mm(u, turn[d])
        for d in range(1, DIAGONALS - 1):
            out = out + mm(gram[d] * u, back[d])
        return out

    step_0 = mu0 / mu1
    next_0 = jnp.maximum(step_0 * step_0 * mu2 - mu0, 0.0)
    grown = 1.0 + next_0 / mu0
    curvature = grown * grown * mu1 - 2.0 * grown * step_0 * mu2 + step_0 * step_0 * mu3
    step_1 = jnp.where(curvature * max_step > next_0, next_0 / curvature, max_step)
    of_r = step_0 + step_1 * grown
    of_v = -step_1 * step_0
    change = of_r * g0 + of_v * g1
    weights = gram_times(coef) + change
    left = coef - weights
    square = mm(left * gram_times(left) + 2.0 * left * change, block)
    square = square + of_r * of_r * mu0 + 2.0 * of_r * of_v * mu1 + of_v * of_v * mu2
    inverse = lax.rsqrt(square + epsilon)
    for s in range(S):
        at = s * K
        x = x0_ref[s].reshape(X * Y, Z) + column(of_r[0:1], at) * r0_ref[s].reshape(X * Y, Z)
        x = x + column(of_v[0:1], at) * v_ref[s].reshape(X * Y, Z)
        out_ref[s] = x.reshape(X, Y, Z)
        rest = (x - weighted(weights[0:1], basis_ref, s)) * column(inverse[0:1], at)
        new_ref[s] = rest.reshape(X, Y, Z).astype(jnp.bfloat16)


def shaped(*shape, dtype=f32):
    return jax.ShapeDtypeStruct(shape, dtype)


def call(kernel, outs, args, small=(), last=False):
    vmem, smem = pl.BlockSpec(memory_space=pltpu.VMEM), pl.BlockSpec(memory_space=pltpu.SMEM)
    specs = jax.tree.map(lambda _: vmem, outs)
    if not last:
        outs = jax.tree.map(lambda out: pltpu.VMEM(out.shape, out.dtype), outs)
    args = [a if i in small else pltpu.with_memory_space_constraint(a, pltpu.VMEM) for i, a in enumerate(args)]
    return pl.pallas_call(
        kernel,
        out_shape=outs,
        in_specs=[smem if i in small else vmem for i in range(len(args))],
        out_specs=specs,
    )(*args)


def total(copies):
    width = copies.shape[2]
    copies = lax.all_to_all(copies, PLANE, 0, 0)
    copies = call(fold_kernel, shaped(lax.axis_size(LINE), 1, width), (copies,))
    return lax.all_to_all(copies, LINE, 0, 0)


def upward(x, axis):
    return lax.ppermute(x, axis, [(i, i + 1) for i in range(lax.axis_size(axis) - 1)])


def downward(x, axis):
    return lax.ppermute(x, axis, [(i + 1, i) for i in range(lax.axis_size(axis) - 1)])


def on_device(rhs, basis, inertia, helm, stiffness):
    scale = 1.0 / float(rhs[0].size * lax.axis_size(PLANE + LINE))
    peers = lax.axis_size(PLANE)
    field = shaped(S, X, Y, Z)

    copies = call(coef_kernel, shaped(peers, 1, Z), (rhs, basis))
    sums = total(copies)

    def start(*refs):
        start_kernel(scale, *refs)

    coef, x0, q, plane, line, up, down = call(
        start,
        (shaped(1, Z), field, field, shaped(X * Y, X * Y), shaped(Z, Z), shaped(2, S, Y, Z), shaped(2, S, Y, Z)),
        (sums, basis, rhs, inertia, helm, stiffness), small=(4,))
    xlo, xhi = upward(up, GX), downward(down, GX)
    up, down = call(y_kernel, (shaped(2 * SX + 8, Z),) * 2, (x0, q, xlo, xhi))
    ylo, yhi = upward(up, "gy"), downward(down, "gy")
    q2, zup, zdown = call(
        z_kernel, (field, shaped(1, 640), shaped(1, 640)), (x0, q, xlo, xhi, ylo, yhi))
    zlo, zhi = upward(zup, "gz"), downward(zdown, "gz")

    places = [(lax.axis_index(axis), lax.axis_size(axis)) for axis in (GX, "gy", "gz")]
    inside = jnp.stack([jnp.where(test, 1.0, 0.0) for i, n in places for test in (i > 0, i < n - 1)])
    r0, v, vx, vy, vz, vz0 = call(
        image_kernel,
        (field, field, shaped(S, Y, Z), shaped(SX, Z), shaped(1, SXY), shaped(1, SXY)),
        (x0, q2, xlo, xhi, ylo, yhi, zlo, zhi, zup, zdown, inside, inertia, helm, plane, line), small=(10, 12))
    lows = [upward(a, axis) for a, axis in ((vx, GX), (vy, "gy"), (vz, "gz"))]
    rows = call(moment_kernel, shaped(256, Z), (r0, v, basis, inertia, helm, plane, line), small=(4,))
    copies = call(cross_kernel, shaped(peers, 1, 256), (rows, v, vz0, *lows))
    sums = total(copies)

    def final(*refs):
        final_kernel(scale, *refs)

    return call(final, (field, shaped(S, X, Y, Z, dtype=jnp.bfloat16)), (sums, coef, x0, r0, v, basis), last=True)


def solution(mesh):
    torus = Mesh(
        mesh.devices.reshape(mesh.shape["gx"] // 2, 2, mesh.shape["gy"], mesh.shape["gz"]),
        ("gx_0", "gx_1", "gy", "gz"),
    )
    placed = (P(None, GX, "gy", "gz"), P(None, None, GX, "gy", "gz"), P(GX, "gy", "gz"), P(), P())
    return jax.shard_map(
        on_device,
        mesh=torus,
        in_specs=placed,
        out_specs=(P(None, GX, "gy", "gz"), P(None, GX, "gy", "gz")),
        check_vma=False,
    )
```
